32 devices in a mesh: grp: 4 (over x, core), emb: 8 (over z, y).
Axes of the slice: x: 2, y: 2, z: 4, core: 2. Of those that a mesh axis runs over, the one named last changes fastest.
Arguments:
- indices: int32 [4, 8, 1024, 512], P(None, None, ('grp', 'emb')), may hold values from 0 to 255
- lengths: int32 [4, 1024, 512], P(None, ('grp', 'emb')), may hold values from 1 to 8
- dense: bfloat16 [4, 1024, 128], P(None, ('grp', 'emb')), may hold values from -6 to 6
- tables: bfloat16 [512, 256, 128], P('emb'), may hold values from -3 to 3
- project: bfloat16 [64, 513], replicated, may hold values from -0.25 to 0.25
- top_weight: bfloat16 [4096, 512], P('grp'), may hold values from -0.09375 to 0.09375
Outputs:
- scores: float32 [4, 1024, 512], P(None, ('grp', 'emb'))
The draws below stay inside these ranges and needn't reach their ends.
Inputs may be any that keep to these rules, and one draw needn't show every extreme that they name: `indices`: a row of the table named by the last dimension; slots at or past the bag's length are ignored.
All inputs are finite; a program needn't handle non-finite values.
Results may differ from the reference program's by a relative error of at most 0.0085.
Values may be sent and summed in bfloat16 or wider, within the bound.
No kernel may reach another device: no remote copies, remote signals or barrier semaphores. Data moves between devices by JAX's collectives and lax.ppermute only.
A program may use at most 128 MiB of HBM per device.

```python
import math
import jax
import jax.numpy as jnp
import numpy as np
from jax import lax

WIDTH = 128
TABLES = 512
ROWS = 256
SLOTS = 8
MICRO = 4
BAT_DEV = 32
PROJ = 64
HIDDEN_SIZE = 512
BATCH = 1024


def set_ends(drawn, own_key, smallest, largest):
    dims = drawn.shape
    spot = [jax.random.randint(jax.random.fold_in(own_key, axis), (), 0, dims[axis]) for axis in range(len(dims))]
    drawn = drawn.at[tuple(spot)].set(smallest)
    longest = dims.index(max(dims))
    spot[longest] = (spot[longest] + 1) % dims[longest]
    return drawn.at[tuple(spot)].set(largest)


def block_scale(key, extent, shards, least, top_value):
    loudness, own = 1.0, jax.random.fold_in(key, 6)
    for axis_at, parts in shards:
        heights = jnp.exp(jax.random.uniform(jax.random.fold_in(own, axis_at), (parts,), jnp.float32, least / len(shards), top_value / len(shards)))
        loudness = loudness * jnp.repeat(heights, extent[axis_at] // parts).reshape([-1 if axis == axis_at else 1 for axis in range(len(extent))])
    return loudness


def rank_table(count, lean):
    weights = [(1 << 20) // math.isqrt(grade ** lean) + 1 for grade in range(1, count + 1)]
    spread = 1 + sum(weights) // (1 << 30)
    return np.cumsum(np.array([max(1, weight // spread) for weight in weights]))


def ranked_ids(stream_key, dims, count, slope):
    listing = rank_table(count, slope)
    ticket = jax.random.randint(jax.random.fold_in(stream_key, 1), dims, 0, int(listing[count - 1]))
    rank = jnp.searchsorted(jnp.asarray(listing, jnp.int32), ticket, side="right")
    return jax.random.permutation(jax.random.fold_in(stream_key, 2), count)[rank].astype(jnp.int32)


def normal_values(stream_key, extent, spread, limit, shards=(), held_as=jnp.bfloat16):
    loudness = block_scale(stream_key, extent, shards, -0.22, 0.18) if shards else 1.0
    values = jax.random.normal(stream_key, extent, jnp.float32) * spread * loudness
    return jnp.minimum(jnp.maximum(values, -limit), limit).astype(held_as)


def setup_inputs(seed: int = 0) -> dict:
    key_list = jax.random.split(jax.random.key(seed), 7)
    indices = set_ends(ranked_ids(key_list[0], (MICRO, SLOTS, BATCH, TABLES), ROWS, 1), jax.random.fold_in(key_list[0], 3), 0, ROWS - 1).astype(jnp.int32)
    lengths = set_ends(jax.random.randint(key_list[1], (MICRO, BATCH, TABLES), 1, SLOTS + 1), jax.random.fold_in(key_list[1], 1), 1, SLOTS).astype(jnp.int32)
    dense = normal_values(key_list[2], (MICRO, BATCH, WIDTH), 1.0, 6.0, ((1, 32),))
    tables = normal_values(key_list[3], (TABLES, ROWS, WIDTH), 0.5, 3.0, ((0, 8),))
    project = normal_values(key_list[4], (PROJ, TABLES + 1), (TABLES + 1) ** -0.5, 0.25)
    top_weight = normal_values(key_list[5], (PROJ * PROJ, HIDDEN_SIZE), (PROJ * PROJ) ** -0.5, 0.09375, ((0, 4),))
    return dict(indices=indices, lengths=lengths, dense=dense, tables=tables, project=project, top_weight=top_weight)


def reference(indices, lengths, dense, tables, project, top_weight):
    bag_rows = jnp.transpose(indices, (0, 2, 1, 3)).reshape(-1, BAT_DEV, SLOTS, TABLES)
    bag_lengths = lengths.reshape(-1, BAT_DEV, TABLES)
    dense_rows = dense.reshape(-1, BAT_DEV, WIDTH)
    table_ids = jnp.arange(TABLES).astype(jnp.int32)
    slot_ids = jnp.arange(SLOTS).astype(jnp.int32)
    mixing = project.astype(jnp.float32)

    def one_block(item):
        rows_here, lens_here, dense_here = item
        live = slot_ids[None, :, None] < lens_here[:, None, :]
        picked = tables[table_ids[None, None, :], rows_here]
        pooled = jnp.sum(jnp.where(live[..., None], picked.astype(jnp.float32), 0.0), axis=1).astype(jnp.bfloat16)
        compressed = jnp.einsum("kt,ntw->nkw", mixing[:, 1:], pooled.astype(jnp.float32))
        compressed = compressed + mixing[:, 0][None, :, None] * dense_here.astype(jnp.float32)[:, None, :]
        compressed = compressed.astype(jnp.bfloat16).astype(jnp.float32)
        inter = (jnp.einsum("nkw,njw->nkj", compressed, compressed) * (WIDTH ** -0.5)).astype(jnp.bfloat16)
        flat = inter.reshape(inter.shape[0], PROJ * PROJ)
        return jnp.dot(flat, top_weight, preferred_element_type=jnp.float32)

    scores = lax.map(one_block, (bag_rows, bag_lengths, dense_rows))
    return scores.reshape(MICRO, BATCH, HIDDEN_SIZE)
```

```python
import functools
import jax
import jax.numpy as jnp
from jax import lax
from jax.experimental import pallas as pl
from jax.experimental.pallas import tpu as pltpu
from jax.sharding import PartitionSpec as P

FIELDS = 8
BITS = 4
PAD = 8
VMEM = pl.BlockSpec(memory_space=pltpu.VMEM)
SMEM = pl.BlockSpec(memory_space=pltpu.SMEM)
ANY = pl.BlockSpec(memory_space=pl.ANY)


def params(mib):
    return pltpu.CompilerParams(vmem_limit_bytes=mib * 2**20)


def cost(us):
    return pl.CostEstimate(flops=int(us * 2e8), bytes_accessed=2**20, transcendentals=0)


def bag_kernel(line, side_ref, indices_ref, lengths_ref, kept_ref, sent_ref):
    micro, slots, batch, table_count = indices_ref.shape
    tab_dev = table_count // line // 2
    side = side_ref[0]
    lengths = jnp.concatenate([lengths_ref[m] for m in range(micro)], axis=0)
    for slot in range(slots):
        picked = jnp.concatenate([indices_ref[m, slot] for m in range(micro)], axis=0)
        turned = jnp.transpose(jnp.where(lengths > slot, picked, -1))
        for block in range(2 * line):
            value = turned[block * tab_dev : (block + 1) * tab_dev]
            rows = pl.ds(block // 2 * tab_dev * slots + slot, tab_dev, stride=slots)

            @pl.when(side == block % 2)
            def _():
                kept_ref[rows, :] = value

            @pl.when(side != block % 2)
            def _():
                sent_ref[rows, :] = value


def make_bags(side, indices, lengths, line):
    micro, slots, batch, table_count = indices.shape
    shape = jax.ShapeDtypeStruct((table_count // 2 * slots, micro * batch), jnp.int32)
    return pl.pallas_call(
        functools.partial(bag_kernel, line),
        out_shape=(shape, shape),
        in_specs=[SMEM, VMEM, VMEM],
        out_specs=(VMEM, VMEM),
        compiler_params=params(32),
        cost_estimate=cost(6),
        name="bags",
    )(side[None], indices, lengths)


def bag_counts(bag, rows):
    slots, samples = bag.shape
    span = rows // FIELDS
    word = bag & (span - 1)
    shift = lax.shift_right_logical(bag, span.bit_length() - 1) * BITS
    step = jnp.where(bag >= 0, lax.shift_left(jnp.ones_like(bag), shift & 31), 0)
    ids = lax.broadcasted_iota(jnp.int32, (span, samples), 0)
    packed = jnp.zeros((span, samples), jnp.int32)
    for slot in range(slots):
        packed = packed + jnp.where(ids == word[slot : slot + 1], step[slot : slot + 1], 0)
    fields = [
        (lax.shift_right_logical(packed, BITS * field) & (2**BITS - 1)).astype(jnp.float32)
        for field in range(FIELDS)
    ]
    return jnp.concatenate([field.astype(jnp.bfloat16) for field in fields], axis=0)


def pool_kernel(first, part, masks, unroll, earlier, places, *refs):
    sources = refs[: len(masks)]
    bags_refs = refs[len(masks) : len(masks) + 2]
    refs = refs[len(masks) + 2 :]
    before = refs[:earlier]
    refs = refs[earlier:]
    if earlier:
        project_ref, mine_ref, theirs_ref = refs[:3]
        tables_ref, bags, low_ref, high_ref, sems, held, sum_ref = refs[3:]
    else:
        (pooled_ref,) = refs[:1]
        tables_ref, bags, low_ref, high_ref, sems = refs[1:]
    tab_dev, _, rows = tables_ref.shape
    slots, samples = bags.shape[2:]
    stride = tab_dev + PAD
    halves = (low_ref, high_ref)

    copies = []
    for number, source in enumerate(bags_refs):
        rows_from = source.at[pl.ds(places[0] * tab_dev, tab_dev)]
        copies.append(pltpu.make_async_copy(rows_from, bags.at[number], sems.at[number]))
    groups = []
    for number, (source, group) in enumerate(zip(sources, masks)):
        size = tab_dev // (len(masks) * len(group))
        sem = sems.at[2 + number]
        if source.shape[1] != part:
            source = source.at[:, pl.ds(first, part)]
        moves = []
        for index, mask in enumerate(group):
            start = (places[1] ^ mask) * size
            moves.append(
                pltpu.make_async_copy(
                    source.at[pl.ds(index * size, size)], tables_ref.at[pl.ds(start, size)], sem
                )
            )
        groups.append((moves, [((places[1] ^ mask) * size, size) for mask in group]))
    late = [
        pltpu.make_async_copy(source, held.at[number], sems.at[2 + len(masks) + number])
        for number, source in enumerate(before)
    ]
    for copy in copies + [move for moves, _ in groups for move in moves] + late:
        copy.start()
    for copy in copies:
        copy.wait()

    for number, (moves, spans) in enumerate(groups):
        whole = tables_ref.at[pl.ds(0, sum(size for _, size in spans))]
        pltpu.make_async_copy(whole, whole, sems.at[2 + number]).wait()
        for base, size in spans:
            times = min(unroll, size)

            def some_tables(step, carry):
                for inner in range(times):
                    table = base + step * times + inner
                    counts = jnp.concatenate(
                        [bag_counts(bags[half, table], rows) for half in range(2)], axis=1
                    )
                    pooled = jnp.dot(tables_ref[table], counts, preferred_element_type=jnp.float32)
                    for half in range(2):
                        halves[half][pl.ds(table, part, stride=stride), :] = pooled[
                            :, half * samples : (half + 1) * samples
                        ]
                return carry

            lax.fori_loop(0, size // times, some_tables, 0)

    if not earlier:

        def narrow(step, carry):
            for inner in range(4):
                column = step * 4 + inner
                start = pl.multiple_of(column * stride, PAD)
                for half in range(2):
                    value = halves[half][pl.ds(start, tab_dev), :].astype(jnp.bfloat16)
                    pooled_ref[column, :, half * samples : (half + 1) * samples] = value
            return carry

        lax.fori_loop(0, part // 4, narrow, 0)
        return

    outs = project_ref.shape[0]
    for copy in late:
        copy.wait()

    def some_columns(step, carry):
        for inner in range(4):
            column = step * 4 + inner
            start = pl.multiple_of(column * stride, PAD)
            own = [ref[pl.ds(start, tab_dev), :].astype(jnp.bfloat16) for ref in halves]
            pooled = jnp.concatenate(
                [held[number, column] for number in range(earlier)]
                + [jnp.concatenate(own, axis=1)],
                axis=0,
            )
            total = jnp.dot(project_ref[...], pooled, preferred_element_type=jnp.float32)
            mine_ref[pl.ds(column, outs, stride=part), :] = total[:, :samples]
            sum_ref[pl.ds(column, outs, stride=part), :] = total[:, samples:]
        return carry

    lax.fori_loop(0, part // 4, some_columns, 0)
    theirs_ref[...] = sum_ref[...].astype(theirs_ref.dtype)


def pool_block(first, part, place, sources, masks, bags, tab_dev, earlier=(), project=None):
    rows = sources[0].shape[2]
    _, slots, samples = bags[0].shape
    scratch = [
        pltpu.VMEM((tab_dev, part, rows), jnp.bfloat16),
        pltpu.VMEM((2, tab_dev, slots, samples), jnp.int32),
        pltpu.VMEM((part * (tab_dev + PAD), samples), jnp.float32),
        pltpu.VMEM((part * (tab_dev + PAD), samples), jnp.float32),
        pltpu.SemaphoreType.DMA((2 + len(masks) + len(earlier),)),
    ]
    if earlier:
        outs = project.shape[0]
        out_shape = (
            jax.ShapeDtypeStruct((outs * part, samples), jnp.float32),
            jax.ShapeDtypeStruct((outs * part, samples), jnp.bfloat16),
        )
        out_specs = (VMEM, VMEM)
        scratch += [
            pltpu.VMEM((len(earlier), part, tab_dev, 2 * samples), jnp.bfloat16),
            pltpu.VMEM((outs * part, samples), jnp.float32),
        ]
        more, specs, time = (project,), [VMEM], 14
    else:
        out_shape = jax.ShapeDtypeStruct((part, tab_dev, 2 * samples), jnp.bfloat16)
        out_specs, more, specs, time = VMEM, (), [], 9
    return pl.pallas_call(
        functools.partial(pool_kernel, first, part, masks, 4, len(earlier)),
        out_shape=out_shape,
        in_specs=[SMEM] + [ANY] * (len(sources) + 2 + len(earlier)) + specs,
        out_specs=out_specs,
        scratch_shapes=scratch,
        compiler_params=params(40),
        cost_estimate=cost(time),
        name="project" if earlier else "pool",
    )(place, *sources, *bags, *earlier, *more)


def score_kernel(masks, scale, member_ref, lead_ref, dense_ref, *refs):
    parts = len(refs) - len(masks) - 5
    sums = refs[:parts]
    top_parts = refs[parts : parts + len(masks)]
    scores_ref, turned, inter, top, sems = refs[parts + len(masks) :]
    own, back = sums[: parts // 2], sums[parts // 2 :]
    width, samples = dense_ref.shape
    outs = lead_ref.shape[0]
    half = outs // 2
    step_k, step_b = outs + PAD, samples + PAD
    copies = []
    for number, (mask, source) in enumerate(zip(masks, top_parts)):
        rows = source.shape[0]
        target = top.at[pl.ds((member_ref[0] ^ mask[0]) * mask[1] + mask[2], rows)]
        copies.append(pltpu.make_async_copy(source, target, sems.at[number]))
    for copy in copies:
        copy.start()

    def compress(step, carry):
        for inner in range(4):
            k = step * 4 + inner
            columns = []
            for mine, theirs in zip(own, back):
                part = mine.shape[0] // outs
                rows = pl.ds(pl.multiple_of(k * part, part), part)
                columns.append(mine[rows, :] + theirs[rows, :].astype(jnp.float32))
            value = jnp.concatenate(columns, axis=0) + lead_ref[k] * dense_ref[...]
            value = jnp.transpose(value).astype(jnp.bfloat16).astype(jnp.float32)
            turned[pl.ds(k, samples, stride=step_k), :] = value
        return carry

    lax.fori_loop(0, outs // 4, compress, 0)

    def interact(step, carry):
        for inner in range(4):
            b = step * 4 + inner
            value = turned[pl.ds(pl.multiple_of(b * step_k, PAD), outs), :].astype(jnp.bfloat16)
            zero = jnp.zeros_like(value)
            left = jnp.concatenate([value[:half], value[half:]], axis=1)
            right = jnp.concatenate(
                [jnp.concatenate([value, zero], axis=1), jnp.concatenate([zero, value], axis=1)],
                axis=0,
            )
            pairs = lax.dot_general(
                left, right, (((1,), (1,)), ((), ())), preferred_element_type=jnp.float32
            )
            inter[pl.ds(b, half, stride=step_b), :] = pairs * scale
        return carry

    lax.fori_loop(0, samples // 4, interact, 0)
    for copy in copies:
        copy.wait()
    scores_ref[...] = jnp.zeros_like(scores_ref)

    def score(step, carry):
        left, right = [], []
        for inner in range(2):
            k = step * 2 + inner
            rows = pl.ds(pl.multiple_of(k * step_b, PAD), samples)
            left.append(inter[rows, :].astype(jnp.bfloat16))
            for high in range(2):
                start = pl.multiple_of((high * half + k) * outs, outs)
                right.append(top[pl.ds(start, outs), :])
        scores_ref[...] += jnp.dot(
            jnp.concatenate(left, axis=1),
            jnp.concatenate(right, axis=0),
            preferred_element_type=jnp.float32,
        )
        return carry

    lax.fori_loop(0, half // 2, score, 0)


def make_scores(member, lead, dense, own, back, tops, masks, top_shape):
    width, samples = dense.shape
    outs = lead.shape[0]
    return pl.pallas_call(
        functools.partial(score_kernel, masks, width ** (-0.5)),
        out_shape=jax.ShapeDtypeStruct((samples, top_shape[1]), jnp.float32),
        in_specs=[SMEM, SMEM, VMEM] + [VMEM] * (2 * len(own)) + [ANY] * len(tops),
        out_specs=VMEM,
        scratch_shapes=[
            pltpu.VMEM((samples * (outs + PAD), width), jnp.float32),
            pltpu.VMEM((outs // 2 * (samples + PAD), 2 * outs), jnp.float32),
            pltpu.VMEM(top_shape, jnp.bfloat16),
            pltpu.SemaphoreType.DMA((len(tops),)),
        ],
        compiler_params=params(40),
        cost_estimate=cost(20),
        name="scores",
    )(member[None], lead, dense, *own, *back, *tops)


def swap(value, axis, size, distance, keep=None, scale=1):
    pairs = []
    for a in range(size):
        if keep is None or keep(a, a ^ distance):
            pairs += [(a * scale + low, (a ^ distance) * scale + low) for low in range(scale)]
    return lax.ppermute(value, axis, pairs)


def line_slot(value, slots, distance, line, position):
    if distance < 3 or distance % 2 == 0:
        return swap(value, "emb", line, distance, None, 2)
    near = lambda a, b: abs(a - b) == 1
    direct = swap(value, "emb", line, distance, near, 2)
    far = lambda a, b: abs(b - (b ^ distance)) != 1
    routed = swap(slots[distance - 2], "emb", line, 1, far, 2)
    adjacent = jnp.abs(position - (position ^ distance)) == 1
    return jnp.where(adjacent, direct, routed)


def share(value, size):
    bit, masks = size // 2, [0]
    while bit > 1:
        value = jnp.concatenate([value, swap(value, "grp", size, bit)], axis=0)
        masks = masks + [mask ^ bit for mask in masks]
        bit //= 2
    if not bit:
        return [value], [masks]
    return [value, swap(value, "grp", size, 1)], [masks, [mask ^ 1 for mask in masks]]


def shards(grp, emb, indices, lengths, dense, tables, project, top_weight):
    micro, slot_count, batch, table_count = indices.shape
    tab_dev, rows, width = tables.shape
    outs = project.shape[0]
    samples = micro * batch
    line = emb // 2
    place = lax.axis_index("emb").astype(jnp.int32)
    member = lax.axis_index("grp").astype(jnp.int32)
    position, side = place // 2, place % 2
    size = tab_dev // grp
    widths = (width // 2, width // 2) if size * rows >= 4096 else (width,)

    mine = lax.dynamic_slice_in_dim(tables, member * size, size, 0)
    mine = jnp.transpose(mine, (0, 2, 1))
    starts = [sum(widths[:number]) for number in range(len(widths))]
    sends = [mine[:, first : first + part] for first, part in zip(starts, widths)]

    top_rows = top_weight.shape[0]
    tops, top_masks = [top_weight], [(0, top_rows, 0)]
    bit = grp // 2
    while bit:
        moved = [swap(piece, "grp", grp, bit) for piece in tops]
        tops = tops + moved
        top_masks = top_masks + [(mask ^ bit, step, start) for mask, step, start in top_masks]
        bit //= 2

    kept, sent = make_bags(side, indices, lengths, line)
    got = swap(sent, "emb", emb, 1)
    bags = [bag.reshape(line * tab_dev, slot_count, samples) for bag in (kept, got)]

    block = jnp.transpose(tables, (0, 2, 1))
    mixing = project[:, 1:].reshape(outs, line, 2, tab_dev)
    mixing = lax.dynamic_index_in_dim(mixing, side, 2, keepdims=False)
    order = position ^ jnp.arange(line)
    mixing = jnp.take(mixing, order, axis=1).reshape(outs, line * tab_dev)

    own, back = [], []
    for first, part, send in zip(starts, widths, sends):
        slots = []
        for distance in range(1, line):
            slots.append(line_slot(send, slots, distance, line, position))
        pooled = []
        for distance in range(line):
            where = jnp.stack([position ^ distance, member if distance else member * 0])
            if distance:
                sources, masks = share(slots[distance - 1], grp)
            else:
                sources, masks = [block], [[0]]
            last = distance == line - 1
            pooled.append(
                pool_block(
                    first,
                    part,
                    where,
                    sources,
                    masks,
                    bags,
                    tab_dev,
                    tuple(pooled) if last else (),
                    mixing if last else None,
                )
            )
        mine_sum, their_sum = pooled[-1]
        own.append(mine_sum)
        back.append(swap(their_sum, "emb", emb, 1))

    flat_dense = jnp.transpose(dense.reshape(samples, width)).astype(jnp.float32)
    lead = project[:, 0].astype(jnp.float32)
    top_shape = (top_rows * grp, top_weight.shape[1])
    scores = make_scores(member, lead, flat_dense, own, back, tops, tuple(top_masks), top_shape)
    return scores.reshape(micro, batch, -1)


def solution(mesh):
    placed = (
        P(None, None, ("grp", "emb"), None),
        P(None, ("grp", "emb"), None),
        P(None, ("grp", "emb"), None),
        P("emb", None, None),
        P(),
        P("grp", None),
    )
    body = functools.partial(shards, mesh.shape["grp"], mesh.shape["emb"])
    return jax.shard_map(
        body, mesh=mesh, in_specs=placed, out_specs=P(None, ("grp", "emb"), None), check_vma=False
    )
```

```python
import functools
import jax
import jax.numpy as jnp
from jax import lax
from jax.experimental import pallas as pl
from jax.experimental.pallas import tpu as pltpu
from jax.sharding import PartitionSpec as P

FIELDS = 8
BITS = 4
PAD = 8
SPLIT = 5
VMEM = pl.BlockSpec(memory_space=pltpu.VMEM)
SMEM = pl.BlockSpec(memory_space=pltpu.SMEM)
ANY = pl.BlockSpec(memory_space=pl.ANY)


def params(mib):
    return pltpu.CompilerParams(vmem_limit_bytes=mib * 2**20)


def cost(us):
    return pl.CostEstimate(flops=int(us * 2e8), bytes_accessed=2**20, transcendentals=0)


def bag_kernel(line, side_ref, indices_ref, lengths_ref, kept_ref, sent_ref):
    micro, slots, _, table_count = indices_ref.shape
    tab_dev = table_count // line // 2
    side = side_ref[0]
    lengths = jnp.concatenate([lengths_ref[m] for m in range(micro)], axis=0)
    pairs = slots // 2
    for pair in range(pairs):
        words = []
        for slot in (pair, pair + pairs):
            picked = jnp.concatenate([indices_ref[m, slot] for m in range(micro)], axis=0)
            words.append(jnp.where(lengths > slot, picked, -1))
        turned = jnp.transpose((words[0] & 0xFFFF) | lax.shift_left(words[1], 16))
        for block in range(2 * line):
            value = turned[block * tab_dev : (block + 1) * tab_dev]
            rows = pl.ds(block // 2 * tab_dev * pairs + pair, tab_dev, stride=pairs)

            @pl.when(side == block % 2)
            def _():
                kept_ref[rows, :] = value

            @pl.when(side != block % 2)
            def _():
                sent_ref[rows, :] = value


def make_bags(side, indices, lengths, line):
    micro, slots, batch, table_count = indices.shape
    shape = jax.ShapeDtypeStruct((table_count // 2 * (slots // 2), micro * batch), jnp.int32)
    return pl.pallas_call(
        functools.partial(bag_kernel, line),
        out_shape=(shape, shape),
        in_specs=[SMEM, VMEM, VMEM],
        out_specs=(VMEM, VMEM),
        compiler_params=params(32),
        cost_estimate=cost(6),
        name="bags",
    )(side[None], indices, lengths)


def turn_kernel(cuts, member_ref, tables_ref, *refs):
    outs, (held, sem) = refs[: len(cuts)], refs[len(cuts) :]
    size = held.shape[0]
    copy = pltpu.make_async_copy(tables_ref.at[pl.ds(member_ref[0] * size, size)], held, sem)
    copy.start()
    copy.wait()
    for table in range(size):
        turned = jnp.transpose(held[table])
        for (first, part), out in zip(cuts, outs):
            out[table] = turned[first : first + part]


def turn_piece(member, tables, size, cuts):
    _, rows, width = tables.shape
    return pl.pallas_call(
        functools.partial(turn_kernel, cuts),
        out_shape=[jax.ShapeDtypeStruct((size, part, rows), tables.dtype) for _, part in cuts],
        in_specs=[SMEM, ANY],
        out_specs=[VMEM] * len(cuts),
        scratch_shapes=[pltpu.VMEM((size, rows, width), tables.dtype), pltpu.SemaphoreType.DMA(())],
        compiler_params=params(63),
        cost_estimate=cost(3),
        name="turn",
    )(member[None], tables)


def bag_counts(bag, rows):
    bag = jnp.concatenate(
        [lax.shift_right_arithmetic(lax.shift_left(bag, 16), 16), lax.shift_right_arithmetic(bag, 16)],
        axis=0,
    )
    slots, samples = bag.shape
    span = rows // FIELDS
    word = bag & (span - 1)
    shift = lax.shift_right_logical(bag, span.bit_length() - 1) * BITS
    step = jnp.where(bag >= 0, lax.shift_left(jnp.ones_like(bag), shift & 31), 0)
    ids = lax.broadcasted_iota(jnp.int32, (span, samples), 0)
    packed = jnp.zeros((span, samples), jnp.int32)
    for slot in range(slots):
        packed = packed + jnp.where(ids == word[slot : slot + 1], step[slot : slot + 1], 0)
    fields = [
        (lax.shift_right_logical(packed, BITS * field) & (2**BITS - 1)).astype(jnp.float32)
        for field in range(FIELDS)
    ]
    return jnp.concatenate([field.astype(jnp.bfloat16) for field in fields], axis=0)


def pool_kernel(first, blocks, pieces, size, unroll, earlier, own, places, *refs):
    sources = refs[: len(pieces)]
    bags_refs = refs[len(pieces) : len(pieces) + 2]
    refs = refs[len(pieces) + 2 :]
    before = refs[:earlier]
    refs = refs[earlier:]
    if earlier:
        project_ref, mine_ref, theirs_ref = refs[:3]
        tables_ref, bags, low_ref, high_ref, sems, sum_ref = refs[3:9]
        held = refs[9:]
        part = held[0].shape[0]
    else:
        (pooled_ref,) = refs[:1]
        tables_ref, bags, low_ref, high_ref, sems = refs[1:]
        part = pooled_ref.shape[0]
    count = tables_ref.shape[0]
    tab_dev = count // blocks
    rows = tables_ref.shape[1 if own else 2]
    samples = bags.shape[3]
    stride = count + PAD
    halves = (low_ref, high_ref)
    member = places[blocks]

    soon, later = [], []
    for number, source in enumerate(bags_refs):
        for block in range(blocks):
            rows_from = source.at[pl.ds(places[block] * tab_dev, tab_dev)]
            target = bags.at[number, pl.ds(block * tab_dev, tab_dev)]
            copy = pltpu.make_async_copy(rows_from, target, sems.at[number * blocks + block])
            (later if block else soon).append(copy)
    sem = 2 * blocks
    for source, (block, mask) in zip(sources, pieces):
        target = tables_ref.at[pl.ds(block * tab_dev + (member ^ mask) * size, size)]
        copy = pltpu.make_async_copy(source, target, sems.at[sem])
        (later if block or mask else soon).append(copy)
        sem += 1
    late = []
    for number, source in enumerate(before):
        columns = source.at[pl.ds(first if source.shape[0] != part else 0, part)]
        late.append(pltpu.make_async_copy(columns, held[number], sems.at[sem + number]))
    for copy in soon + later + late:
        copy.start()
    for copy in soon:
        copy.wait()

    base = member * size

    def some_tables(step, carry):
        if later:

            @pl.when(step == size // unroll)
            def _():
                for copy in later:
                    copy.wait()

        at = lax.rem(base + step * unroll, count)
        for inner in range(unroll):
            table = at + inner
            counts = jnp.concatenate(
                [bag_counts(bags[half, table], rows) for half in range(2)], axis=1
            )
            pooled = lax.dot_general(
                tables_ref[table],
                counts,
                (((0 if own else 1,), (0,)), ((), ())),
                preferred_element_type=jnp.float32,
            )
            for half in range(2):
                halves[half][pl.ds(table, part, stride=stride), :] = pooled[
                    :, half * samples : (half + 1) * samples
                ]
        return carry

    lax.fori_loop(0, count // unroll, some_tables, 0)

    if not earlier:

        def narrow(step, carry):
            for inner in range(4):
                column = step * 4 + inner
                start = pl.multiple_of(column * stride, PAD)
                for half in range(2):
                    value = halves[half][pl.ds(start, count), :].astype(jnp.bfloat16)
                    pooled_ref[column, :, half * samples : (half + 1) * samples] = value
            return carry

        lax.fori_loop(0, part // 4, narrow, 0)
        return

    outs = project_ref.shape[0]
    for copy in late:
        copy.wait()

    def some_columns(step, carry):
        for inner in range(4):
            column = step * 4 + inner
            start = pl.multiple_of(column * stride, PAD)
            here = [ref[pl.ds(start, count), :].astype(jnp.bfloat16) for ref in halves]
            pooled = jnp.concatenate(
                [ref[column] for ref in held] + [jnp.concatenate(here, axis=1)], axis=0
            )
            total = jnp.dot(project_ref[...], pooled, preferred_element_type=jnp.float32)
            mine_ref[pl.ds(column, outs, stride=part), :] = total[:, :samples]
            sum_ref[pl.ds(column, outs, stride=part), :] = total[:, samples:]
        return carry

    lax.fori_loop(0, part // 4, some_columns, 0)
    theirs_ref[...] = sum_ref[...].astype(theirs_ref.dtype)


def pool_blocks(places, sources, pieces, bags, tab_dev, part, first=0, earlier=(), project=None):
    own = project is None and sources[0].shape[0] == tab_dev
    blocks = places.shape[0] - 1
    count = blocks * tab_dev
    size = sources[0].shape[0]
    rows = sources[0].shape[1 if own else 2]
    _, pairs, samples = bags[0].shape
    scratch = [
        pltpu.VMEM((count, rows, part) if own else (count, part, rows), jnp.bfloat16),
        pltpu.VMEM((2, count, pairs, samples), jnp.int32),
        pltpu.VMEM((part * (count + PAD), samples), jnp.float32),
        pltpu.VMEM((part * (count + PAD), samples), jnp.float32),
        pltpu.SemaphoreType.DMA((2 * blocks + len(pieces) + len(earlier),)),
    ]
    if earlier:
        outs = project.shape[0]
        out_shape = (
            jax.ShapeDtypeStruct((outs * part, samples), jnp.float32),
            jax.ShapeDtypeStruct((outs * part, samples), jnp.bfloat16),
        )
        out_specs = (VMEM, VMEM)
        scratch += [pltpu.VMEM((outs * part, samples), jnp.float32)]
        scratch += [pltpu.VMEM((part, *one.shape[1:]), jnp.bfloat16) for one in earlier]
        more, specs = (project,), [VMEM]
    else:
        out_shape = jax.ShapeDtypeStruct((part, count, 2 * samples), jnp.bfloat16)
        out_specs, more, specs = VMEM, (), []
    unroll = min(16, size)
    return pl.pallas_call(
        functools.partial(pool_kernel, first, blocks, pieces, size, unroll, len(earlier), own),
        out_shape=out_shape,
        in_specs=[SMEM] + [ANY] * (len(sources) + 2 + len(earlier)) + specs,
        out_specs=out_specs,
        scratch_shapes=scratch,
        compiler_params=params(63),
        cost_estimate=cost(10),
        name="project" if earlier else "pool",
    )(places, *sources, *bags, *earlier, *more)


def score_kernel(masks, scale, member_ref, lead_ref, dense_ref, *refs):
    parts = len(refs) - len(masks) - 5
    sums = refs[:parts]
    top_parts = refs[parts : parts + len(masks)]
    scores_ref, turned, inter, top, sems = refs[parts + len(masks) :]
    own, back = sums[: parts // 2], sums[parts // 2 :]
    _, samples = dense_ref.shape
    outs = lead_ref.shape[0]
    half = outs // 2
    step_k, step_b = outs + PAD, samples + PAD
    copies = []
    for number, (mask, source) in enumerate(zip(masks, top_parts)):
        rows = source.shape[0]
        target = top.at[pl.ds((member_ref[0] ^ mask) * rows, rows)]
        copies.append(pltpu.make_async_copy(source, target, sems.at[number]))
    for copy in copies:
        copy.start()

    def compress(step, carry):
        for inner in range(4):
            k = step * 4 + inner
            columns = []
            for mine, theirs in zip(own, back):
                part = mine.shape[0] // outs
                rows = pl.ds(pl.multiple_of(k * part, part), part)
                columns.append(mine[rows, :] + theirs[rows, :].astype(jnp.float32))
            value = jnp.concatenate(columns, axis=0) + lead_ref[k] * dense_ref[...]
            value = jnp.transpose(value).astype(jnp.bfloat16).astype(jnp.float32)
            turned[pl.ds(k, samples, stride=step_k), :] = value
        return carry

    lax.fori_loop(0, outs // 4, compress, 0)

    def interact(step, carry):
        for inner in range(4):
            b = step * 4 + inner
            value = turned[pl.ds(pl.multiple_of(b * step_k, PAD), outs), :].astype(jnp.bfloat16)
            zero = jnp.zeros_like(value)
            left = jnp.concatenate([value[:half], value[half:]], axis=1)
            right = jnp.concatenate(
                [jnp.concatenate([value, zero], axis=1), jnp.concatenate([zero, value], axis=1)],
                axis=0,
            )
            pairs = lax.dot_general(
                left, right, (((1,), (1,)), ((), ())), preferred_element_type=jnp.float32
            )
            inter[pl.ds(b, half, stride=step_b), :] = pairs * scale
        return carry

    lax.fori_loop(0, samples // 4, interact, 0)
    for copy in copies:
        copy.wait()
    scores_ref[...] = jnp.zeros_like(scores_ref)

    def score(step, carry):
        left, right = [], []
        for inner in range(2):
            k = step * 2 + inner
            rows = pl.ds(pl.multiple_of(k * step_b, PAD), samples)
            left.append(inter[rows, :].astype(jnp.bfloat16))
            for high in range(2):
                start = pl.multiple_of((high * half + k) * outs, outs)
                right.append(top[pl.ds(start, outs), :])
        scores_ref[...] += jnp.dot(
            jnp.concatenate(left, axis=1),
            jnp.concatenate(right, axis=0),
            preferred_element_type=jnp.float32,
        )
        return carry

    lax.fori_loop(0, half // 2, score, 0)


def make_scores(place, lead, dense, own, back, tops, masks, top_shape):
    width, samples = dense.shape
    outs = lead.shape[0]
    return pl.pallas_call(
        functools.partial(score_kernel, masks, width ** (-0.5)),
        out_shape=jax.ShapeDtypeStruct((samples, top_shape[1]), jnp.float32),
        in_specs=[SMEM, SMEM, VMEM] + [VMEM] * (2 * len(own)) + [ANY] * len(tops),
        out_specs=VMEM,
        scratch_shapes=[
            pltpu.VMEM((samples * (outs + PAD), width), jnp.float32),
            pltpu.VMEM((outs // 2 * (samples + PAD), 2 * outs), jnp.float32),
            pltpu.VMEM(top_shape, jnp.bfloat16),
            pltpu.SemaphoreType.DMA((len(tops),)),
        ],
        compiler_params=params(40),
        cost_estimate=cost(20),
        name="scores",
    )(place, lead, dense, *own, *back, *tops)


def swap(value, axis, size, distance, keep=None, scale=1):
    pairs = []
    for a in range(size):
        if keep is None or keep(a, a ^ distance):
            pairs += [(a * scale + low, (a ^ distance) * scale + low) for low in range(scale)]
    return lax.ppermute(value, axis, pairs)


def routed_slot(distance):
    return distance >= 3 and distance % 2 == 1


def line_slot(value, slots, distance, line, position):
    if not routed_slot(distance):
        return swap(value, "emb", line, distance, None, 2)
    near = lambda a, b: abs(a - b) == 1
    direct = swap(value, "emb", line, distance, near, 2)
    far = lambda a, b: abs(b - (b ^ distance)) != 1
    routed = swap(slots[distance - 2], "emb", line, 1, far, 2)
    adjacent = jnp.abs(position - (position ^ distance)) == 1
    return jnp.where(adjacent, direct, routed)


def share(value, size):
    pieces, masks = [value], [0]
    for bit in bits_of(size):
        moved = [swap(piece, "grp", size, bit) for piece in pieces]
        pieces, masks = pieces + moved, masks + [mask ^ bit for mask in masks]
    return pieces, masks


def bits_of(size):
    return [2**power for power in range(size.bit_length() - 2, -1, -1)]


def chunk_widths(width, piece):
    return (width // 8 * SPLIT, width - width // 8 * SPLIT) if piece >= 4096 else (width,)


def shards(grp, emb, indices, lengths, dense, tables, project, top_weight):
    micro, slot_count, batch, _ = indices.shape
    tab_dev, rows, width = tables.shape
    outs = project.shape[0]
    samples = micro * batch
    line = emb // 2
    place = lax.axis_index("emb").astype(jnp.int32)
    member = lax.axis_index("grp").astype(jnp.int32)
    position, side = place // 2, place % 2
    size = tab_dev // grp
    cuts, first = [], 0
    for part in chunk_widths(width, size * rows):
        cuts.append((first, part))
        first += part
    sends = turn_piece(member, tables, size, cuts)

    top_rows = top_weight.shape[0]
    tops, top_masks = [top_weight], [0]
    for bit in bits_of(grp):
        moved = [swap(piece, "grp", grp, bit) for piece in tops]
        tops, top_masks = tops + moved, top_masks + [mask ^ bit for mask in top_masks]

    kept, sent = make_bags(side, indices, lengths, line)
    got = swap(sent, "emb", emb, 1)
    bags = [bag.reshape(line * tab_dev, slot_count // 2, samples) for bag in (kept, got)]

    mixing = project[:, 1:].reshape(outs, line, 2, tab_dev)
    mixing = lax.dynamic_index_in_dim(mixing, side, 2, keepdims=False)
    order = position ^ jnp.arange(line)
    mixing = jnp.take(mixing, order, axis=1).reshape(outs, line * tab_dev)

    where = jnp.stack([position, member * 0])
    near = pool_blocks(where, [tables], [(0, 0)], bags, tab_dev, width)
    own, back = [], []
    for (first, part), send in zip(cuts, sends):
        slots, sources, pieces = [], [], []
        for distance in range(1, line):
            slots.append(line_slot(send, slots, distance, line, position))
            shared, masks = share(slots[-1], grp)
            sources.append(shared)
            pieces.append([(0 if distance == line - 1 else distance - 1, mask) for mask in masks])
        pooled = [near]
        if line > 2:
            where = jnp.concatenate([order[1 : line - 1], member[None]]).astype(jnp.int32)
            pooled.append(
                pool_blocks(where, sum(sources[:-1], []), sum(pieces[:-1], []), bags, tab_dev, part)
            )
        where = jnp.stack([order[line - 1], member]).astype(jnp.int32)
        mine_sum, their_sum = pool_blocks(
            where, sources[-1], pieces[-1], bags, tab_dev, part, first, tuple(pooled), mixing
        )
        own.append(mine_sum)
        back.append(swap(their_sum, "emb", emb, 1))

    flat_dense = jnp.transpose(dense.reshape(samples, width)).astype(jnp.float32)
    lead = project[:, 0].astype(jnp.float32)
    top_shape = (top_rows * grp, top_weight.shape[1])
    scores = make_scores(
        member[None], lead, flat_dense, own, back, tops, tuple(top_masks), top_shape
    )
    return scores.reshape(micro, batch, -1)


def solution(mesh):
    placed = (
        P(None, None, ("grp", "emb"), None),
        P(None, ("grp", "emb"), None),
        P(None, ("grp", "emb"), None),
        P("emb", None, None),
        P(),
        P("grp", None),
    )
    grp, emb = mesh.shape["grp"], mesh.shape["emb"]

    def body(*args):
        return shards(grp, emb, *args)

    step = jax.shard_map(
        body, mesh=mesh, in_specs=placed, out_specs=P(None, ("grp", "emb"), None), check_vma=False
    )

    def run(indices, lengths, dense, tables, project, top_weight):
        args = (indices, lengths, dense, tables, project, top_weight)
        return step(*args)

    return run
```

```python
import functools
import jax
import jax.numpy as jnp
from jax import lax
from jax.experimental import pallas as pl
from jax.experimental.pallas import tpu as pltpu
from jax.sharding import PartitionSpec as P

FIELDS = 8
BITS = 4
PAD = 8
SPLIT = 5
VMEM = pl.BlockSpec(memory_space=pltpu.VMEM)
SMEM = pl.BlockSpec(memory_space=pltpu.SMEM)
ANY = pl.BlockSpec(memory_space=pl.ANY)


def params(mib):
    return pltpu.CompilerParams(vmem_limit_bytes=mib * 2**20)


def cost(us):
    return pl.CostEstimate(flops=int(us * 2e8), bytes_accessed=2**20, transcendentals=0)


def bag_kernel(line, side_ref, indices_ref, lengths_ref, kept_ref, sent_ref):
    micro, slots, _, table_count = indices_ref.shape
    tab_dev = table_count // line // 2
    side = side_ref[0]
    lengths = jnp.concatenate([lengths_ref[m] for m in range(micro)], axis=0)
    pairs = slots // 2
    for pair in range(pairs):
        words = []
        for slot in (pair, pair + pairs):
            picked = jnp.concatenate([indices_ref[m, slot] for m in range(micro)], axis=0)
            words.append(jnp.where(lengths > slot, picked, -1))
        turned = jnp.transpose((words[0] & 0xFFFF) | lax.shift_left(words[1], 16))
        for block in range(2 * line):
            value = turned[block * tab_dev : (block + 1) * tab_dev]
            rows = pl.ds(block // 2 * tab_dev * pairs + pair, tab_dev, stride=pairs)

            @pl.when(side == block % 2)
            def _():
                kept_ref[rows, :] = value

            @pl.when(side != block % 2)
            def _():
                sent_ref[rows, :] = value


def make_bags(side, indices, lengths, line):
    micro, slots, batch, table_count = indices.shape
    shape = jax.ShapeDtypeStruct((table_count // 2 * (slots // 2), micro * batch), jnp.int32)
    return pl.pallas_call(
        functools.partial(bag_kernel, line),
        out_shape=(shape, shape),
        in_specs=[SMEM, VMEM, VMEM],
        out_specs=(VMEM, VMEM),
        compiler_params=params(32),
        cost_estimate=cost(6),
        name="bags",
    )(side[None], indices, lengths)


def turn_kernel(cuts, member_ref, tables_ref, *refs):
    outs, (held, sem) = refs[: len(cuts)], refs[len(cuts) :]
    size = held.shape[0]
    copy = pltpu.make_async_copy(tables_ref.at[pl.ds(member_ref[0] * size, size)], held, sem)
    copy.start()
    copy.wait()
    for table in range(size):
        turned = jnp.transpose(held[table])
        for (first, part), out in zip(cuts, outs):
            out[table] = turned[first : first + part]


def turn_piece(member, tables, size, cuts):
    _, rows, width = tables.shape
    return pl.pallas_call(
        functools.partial(turn_kernel, cuts),
        out_shape=[jax.ShapeDtypeStruct((size, part, rows), tables.dtype) for _, part in cuts],
        in_specs=[SMEM, ANY],
        out_specs=[VMEM] * len(cuts),
        scratch_shapes=[pltpu.VMEM((size, rows, width), tables.dtype), pltpu.SemaphoreType.DMA(())],
        compiler_params=params(63),
        cost_estimate=cost(3),
        name="turn",
    )(member[None], tables)


def bag_counts(bag, rows):
    bag = jnp.concatenate(
        [lax.shift_right_arithmetic(lax.shift_left(bag, 16), 16), lax.shift_right_arithmetic(bag, 16)],
        axis=0,
    )
    slots, samples = bag.shape
    span = rows // FIELDS
    word = bag & (span - 1)
    shift = lax.shift_right_logical(bag, span.bit_length() - 1) * BITS
    step = jnp.where(bag >= 0, lax.shift_left(jnp.ones_like(bag), shift & 31), 0)
    ids = lax.broadcasted_iota(jnp.int32, (span, samples), 0)
    packed = jnp.zeros((span, samples), jnp.int32)
    for slot in range(slots):
        packed = packed + jnp.where(ids == word[slot : slot + 1], step[slot : slot + 1], 0)
    fields = [
        (lax.shift_right_logical(packed, BITS * field) & (2**BITS - 1)).astype(jnp.float32)
        for field in range(FIELDS)
    ]
    return jnp.concatenate([field.astype(jnp.bfloat16) for field in fields], axis=0)


def pool_kernel(first, distances, pieces, size, unroll, earlier, own, places, *refs):
    sources = refs[: len(pieces)]
    bags_refs = refs[len(pieces) : len(pieces) + 2]
    refs = refs[len(pieces) + 2 :]
    before = refs[:earlier]
    refs = refs[earlier:]
    if earlier:
        project_ref, mine_ref, theirs_ref = refs[:3]
        tables_ref, bags, low_ref, high_ref, sems, sum_ref = refs[3:9]
        held = refs[9:]
        part = held[0].shape[0]
    else:
        (pooled_ref,) = refs[:1]
        tables_ref, bags, low_ref, high_ref, sems = refs[1:]
        part = pooled_ref.shape[0]
    count, blocks = tables_ref.shape[0], len(distances)
    tab_dev = count // blocks
    rows = tables_ref.shape[1 if own else 2]
    samples = bags.shape[3]
    stride = count + PAD
    halves = (low_ref, high_ref)
    member = places[1] * (0 if own else 1)

    soon, later = [], []
    for number, source in enumerate(bags_refs):
        for block in range(blocks):
            rows_from = source.at[pl.ds((places[0] ^ distances[block]) * tab_dev, tab_dev)]
            target = bags.at[number, pl.ds(block * tab_dev, tab_dev)]
            copy = pltpu.make_async_copy(rows_from, target, sems.at[number * blocks + block])
            (later if block else soon).append(copy)
    sem = 2 * blocks
    for source, (block, mask) in zip(sources, pieces):
        target = tables_ref.at[pl.ds(block * tab_dev + (member ^ mask) * size, size)]
        copy = pltpu.make_async_copy(source, target, sems.at[sem])
        (later if block or mask else soon).append(copy)
        sem += 1
    late = []
    for number, source in enumerate(before):
        columns = source.at[pl.ds(first if source.shape[0] != part else 0, part)]
        late.append(pltpu.make_async_copy(columns, held[number], sems.at[sem + number]))
    for copy in soon + later + late:
        copy.start()
    for copy in soon:
        copy.wait()

    base = member * size

    def some_tables(step, carry):
        if later:

            @pl.when(step == size // unroll)
            def _():
                for copy in later:
                    copy.wait()

        at = lax.rem(base + step * unroll, count)
        for inner in range(unroll):
            table = at + inner
            counts = jnp.concatenate(
                [bag_counts(bags[half, table], rows) for half in range(2)], axis=1
            )
            pooled = lax.dot_general(
                tables_ref[table],
                counts,
                (((0 if own else 1,), (0,)), ((), ())),
                preferred_element_type=jnp.float32,
            )
            for half in range(2):
                halves[half][pl.ds(table, part, stride=stride), :] = pooled[
                    :, half * samples : (half + 1) * samples
                ]
        return carry

    lax.fori_loop(0, count // unroll, some_tables, 0)

    if not earlier:

        def narrow(step, carry):
            for inner in range(4):
                column = step * 4 + inner
                start = pl.multiple_of(column * stride, PAD)
                for half in range(2):
                    value = halves[half][pl.ds(start, count), :].astype(jnp.bfloat16)
                    pooled_ref[column, :, half * samples : (half + 1) * samples] = value
            return carry

        lax.fori_loop(0, part // 4, narrow, 0)
        return

    outs = project_ref.shape[0]
    for copy in late:
        copy.wait()

    def some_columns(step, carry):
        for inner in range(4):
            column = step * 4 + inner
            start = pl.multiple_of(column * stride, PAD)
            here = [ref[pl.ds(start, count), :].astype(jnp.bfloat16) for ref in halves]
            pooled = jnp.concatenate(
                [ref[column] for ref in held] + [jnp.concatenate(here, axis=1)], axis=0
            )
            total = jnp.dot(project_ref[...], pooled, preferred_element_type=jnp.float32)
            mine_ref[pl.ds(column, outs, stride=part), :] = total[:, :samples]
            sum_ref[pl.ds(column, outs, stride=part), :] = total[:, samples:]
        return carry

    lax.fori_loop(0, part // 4, some_columns, 0)
    theirs_ref[...] = sum_ref[...].astype(theirs_ref.dtype)


def pool_blocks(
    places, distances, sources, pieces, bags, tab_dev, part, first=0, earlier=(), project=None
):
    own = distances == [0]
    blocks = len(distances)
    count = blocks * tab_dev
    size = sources[0].shape[0]
    rows = sources[0].shape[1 if own else 2]
    _, pairs, samples = bags[0].shape
    scratch = [
        pltpu.VMEM((count, rows, part) if own else (count, part, rows), jnp.bfloat16),
        pltpu.VMEM((2, count, pairs, samples), jnp.int32),
        pltpu.VMEM((part * (count + PAD), samples), jnp.float32),
        pltpu.VMEM((part * (count + PAD), samples), jnp.float32),
        pltpu.SemaphoreType.DMA((2 * blocks + len(pieces) + len(earlier),)),
    ]
    if earlier:
        outs = project.shape[0]
        out_shape = (
            jax.ShapeDtypeStruct((outs * part, samples), jnp.float32),
            jax.ShapeDtypeStruct((outs * part, samples), jnp.bfloat16),
        )
        out_specs = (VMEM, VMEM)
        scratch += [pltpu.VMEM((outs * part, samples), jnp.float32)]
        scratch += [pltpu.VMEM((part, *one.shape[1:]), jnp.bfloat16) for one in earlier]
        more, specs = (project,), [VMEM]
    else:
        out_shape = jax.ShapeDtypeStruct((part, count, 2 * samples), jnp.bfloat16)
        out_specs, more, specs = VMEM, (), []
    unroll = min(16, size)
    return pl.pallas_call(
        functools.partial(pool_kernel, first, distances, pieces, size, unroll, len(earlier), own),
        out_shape=out_shape,
        in_specs=[SMEM] + [ANY] * (len(sources) + 2 + len(earlier)) + specs,
        out_specs=out_specs,
        scratch_shapes=scratch,
        compiler_params=params(63),
        cost_estimate=cost(10),
        name="project" if earlier else "pool",
    )(places, *sources, *bags, *earlier, *more)


def score_kernel(masks, scale, member_ref, lead_ref, dense_ref, *refs):
    parts = len(refs) - len(masks) - 5
    sums = refs[:parts]
    top_parts = refs[parts : parts + len(masks)]
    scores_ref, turned, inter, top, sems = refs[parts + len(masks) :]
    own, back = sums[: parts // 2], sums[parts // 2 :]
    _, samples = dense_ref.shape
    outs = lead_ref.shape[0]
    half = outs // 2
    step_k, step_b = outs + PAD, samples + PAD
    copies = []
    for number, (mask, source) in enumerate(zip(masks, top_parts)):
        rows = source.shape[0]
        target = top.at[pl.ds((member_ref[0] ^ mask) * rows, rows)]
        copies.append(pltpu.make_async_copy(source, target, sems.at[number]))
    for copy in copies:
        copy.start()

    def compress(step, carry):
        for inner in range(8):
            k = step * 8 + inner
            columns = []
            for mine, theirs in zip(own, back):
                part = mine.shape[0] // outs
                rows = pl.ds(pl.multiple_of(k * part, part), part)
                columns.append(mine[rows, :] + theirs[rows, :].astype(jnp.float32))
            value = jnp.concatenate(columns, axis=0) + lead_ref[k] * dense_ref[...]
            value = jnp.transpose(value).astype(jnp.bfloat16).astype(jnp.float32)
            turned[pl.ds(k, samples, stride=step_k), :] = value
        return carry

    lax.fori_loop(0, outs // 8, compress, 0)

    def interact(step, carry):
        for inner in range(16):
            b = step * 16 + inner
            value = turned[pl.ds(pl.multiple_of(b * step_k, PAD), outs), :].astype(jnp.bfloat16)
            zero = jnp.zeros_like(value)
            left = jnp.concatenate([value[:half], value[half:]], axis=1)
            right = jnp.concatenate(
                [jnp.concatenate([value, zero], axis=1), jnp.concatenate([zero, value], axis=1)],
                axis=0,
            )
            pairs = lax.dot_general(
                left, right, (((1,), (1,)), ((), ())), preferred_element_type=jnp.float32
            )
            inter[pl.ds(b, half, stride=step_b), :] = pairs * scale
        return carry

    lax.fori_loop(0, samples // 16, interact, 0)
    for copy in copies:
        copy.wait()
    scores_ref[...] = jnp.zeros_like(scores_ref)

    def score(step, carry):
        left, right = [], []
        for inner in range(2):
            k = step * 2 + inner
            rows = pl.ds(pl.multiple_of(k * step_b, PAD), samples)
            left.append(inter[rows, :].astype(jnp.bfloat16))
            for high in range(2):
                start = pl.multiple_of((high * half + k) * outs, outs)
                right.append(top[pl.ds(start, outs), :])
        scores_ref[...] += jnp.dot(
            jnp.concatenate(left, axis=1),
            jnp.concatenate(right, axis=0),
            preferred_element_type=jnp.float32,
        )
        return carry

    lax.fori_loop(0, half // 2, score, 0)


def make_scores(place, lead, dense, own, back, tops, masks, top_shape):
    width, samples = dense.shape
    outs = lead.shape[0]
    return pl.pallas_call(
        functools.partial(score_kernel, masks, width ** (-0.5)),
        out_shape=jax.ShapeDtypeStruct((samples, top_shape[1]), jnp.float32),
        in_specs=[SMEM, SMEM, VMEM] + [VMEM] * (2 * len(own)) + [ANY] * len(tops),
        out_specs=VMEM,
        scratch_shapes=[
            pltpu.VMEM((samples * (outs + PAD), width), jnp.float32),
            pltpu.VMEM((outs // 2 * (samples + PAD), 2 * outs), jnp.float32),
            pltpu.VMEM(top_shape, jnp.bfloat16),
            pltpu.SemaphoreType.DMA((len(tops),)),
        ],
        compiler_params=params(40),
        cost_estimate=cost(20),
        name="scores",
    )(place, lead, dense, *own, *back, *tops)


def swap(value, axis, size, distance, keep=None, scale=1):
    pairs = []
    for a in range(size):
        if keep is None or keep(a, a ^ distance):
            pairs += [(a * scale + low, (a ^ distance) * scale + low) for low in range(scale)]
    return lax.ppermute(value, axis, pairs)


def routed_slot(distance):
    return distance >= 3 and distance % 2 == 1


def line_slot(value, slots, distance, line, position):
    if not routed_slot(distance):
        return swap(value, "emb", line, distance, None, 2)
    near = lambda a, b: abs(a - b) == 1
    direct = swap(value, "emb", line, distance, near, 2)
    far = lambda a, b: abs(b - (b ^ distance)) != 1
    routed = swap(slots[distance - 2], "emb", line, 1, far, 2)
    adjacent = jnp.abs(position - (position ^ distance)) == 1
    return jnp.where(adjacent, direct, routed)


def share(value, size):
    pieces, masks = [value], [0]
    for bit in bits_of(size):
        moved = [swap(piece, "grp", size, bit) for piece in pieces]
        pieces, masks = pieces + moved, masks + [mask ^ bit for mask in masks]
    return pieces, masks


def bits_of(size):
    return [2**power for power in range(size.bit_length() - 2, -1, -1)]


def chunk_widths(width, piece):
    return (width // 8 * SPLIT, width - width // 8 * SPLIT) if piece >= 4096 else (width,)


def shards(grp, emb, indices, lengths, dense, tables, project, top_weight):
    micro, slot_count, batch, _ = indices.shape
    tab_dev, rows, width = tables.shape
    outs = project.shape[0]
    samples = micro * batch
    line = emb // 2
    place = lax.axis_index("emb").astype(jnp.int32)
    member = lax.axis_index("grp").astype(jnp.int32)
    position, side = place // 2, place % 2
    size = tab_dev // grp
    cuts, first = [], 0
    for part in chunk_widths(width, size * rows):
        cuts.append((first, part))
        first += part
    sends = turn_piece(member, tables, size, cuts)

    top_rows = top_weight.shape[0]
    tops, top_masks = [top_weight], [0]
    for bit in bits_of(grp):
        moved = [swap(piece, "grp", grp, bit) for piece in tops]
        tops, top_masks = tops + moved, top_masks + [mask ^ bit for mask in top_masks]

    kept, sent = make_bags(side, indices, lengths, line)
    got = swap(sent, "emb", emb, 1)
    bags = [bag.reshape(line * tab_dev, slot_count // 2, samples) for bag in (kept, got)]

    mixing = project[:, 1:].reshape(outs, line, 2, tab_dev)
    mixing = lax.dynamic_index_in_dim(mixing, side, 2, keepdims=False)
    order = position ^ jnp.arange(line)
    mixing = jnp.take(mixing, order, axis=1).reshape(outs, line * tab_dev)

    mixing, where = lax.optimization_barrier((mixing, jnp.stack([position, member])))
    near = pool_blocks(where, [0], [tables], [(0, 0)], bags, tab_dev, width)
    own, back = [], []
    for chunk, ((first, part), send) in enumerate(zip(cuts, sends)):
        slots, sources, pieces = [], [], []
        for distance in range(1, line):
            slots.append(line_slot(send, slots, distance, line, position))
            shared, masks = share(slots[-1], grp)
            sources.append(shared)
            pieces.append([(0 if distance == line - 1 else distance - 1, mask) for mask in masks])
        pooled, groups = [near], [[distance] for distance in range(1, line - 1)]
        if chunk == len(cuts) - 1:
            groups = [sum(groups, [])] if groups else []
        for group in groups:
            arrays = sum([sources[distance - 1] for distance in group], [])
            marks = [(group.index(d), mask) for d in group for _, mask in pieces[d - 1]]
            pooled.append(pool_blocks(where, group, arrays, marks, bags, tab_dev, part))
        mine_sum, their_sum = pool_blocks(
            where,
            [line - 1],
            sources[-1],
            pieces[-1],
            bags,
            tab_dev,
            part,
            first,
            tuple(pooled),
            mixing,
        )
        own.append(mine_sum)
        back.append(swap(their_sum, "emb", emb, 1))

    flat_dense = jnp.transpose(dense.reshape(samples, width)).astype(jnp.float32)
    lead = project[:, 0].astype(jnp.float32)
    top_shape = (top_rows * grp, top_weight.shape[1])
    scores = make_scores(
        member[None], lead, flat_dense, own, back, tops, tuple(top_masks), top_shape
    )
    return scores.reshape(micro, batch, -1)


def solution(mesh):
    placed = (
        P(None, None, ("grp", "emb"), None),
        P(None, ("grp", "emb"), None),
        P(None, ("grp", "emb"), None),
        P("emb", None, None),
        P(),
        P("grp", None),
    )
    grp, emb = mesh.shape["grp"], mesh.shape["emb"]

    def body(*args):
        return shards(grp, emb, *args)

    step = jax.shard_map(
        body, mesh=mesh, in_specs=placed, out_specs=P(None, ("grp", "emb"), None), check_vma=False
    )

    def run(indices, lengths, dense, tables, project, top_weight):
        args = (indices, lengths, dense, tables, project, top_weight)
        return step(*args)

    return run
```

```python
import functools
import jax
import jax.numpy as jnp
from jax import lax
from jax.experimental import pallas as pl
from jax.experimental.pallas import tpu as pltpu
from jax.sharding import PartitionSpec as P

FIELDS = 8
BITS = 4
PAD = 8
SPLIT = 5
VMEM = pl.BlockSpec(memory_space=pltpu.VMEM)
SMEM = pl.BlockSpec(memory_space=pltpu.SMEM)
ANY = pl.BlockSpec(memory_space=pl.ANY)


def params(mib):
    return pltpu.CompilerParams(vmem_limit_bytes=mib * 2**20)


def cost(us):
    return pl.CostEstimate(flops=int(us * 2e8), bytes_accessed=2**20, transcendentals=0)


def bag_kernel(line, side_ref, indices_ref, lengths_ref, kept_ref, sent_ref):
    micro, slots, _, table_count = indices_ref.shape
    tab_dev = table_count // line // 2
    side = side_ref[0]
    lengths = jnp.concatenate([lengths_ref[m] for m in range(micro)], axis=0)
    pairs = slots // 2
    for pair in range(pairs):
        words = []
        for slot in (pair, pair + pairs):
            picked = jnp.concatenate([indices_ref[m, slot] for m in range(micro)], axis=0)
            words.append(jnp.where(lengths > slot, picked, -1))
        turned = jnp.transpose((words[0] & 0xFFFF) | lax.shift_left(words[1], 16))
        for block in range(2 * line):
            value = turned[block * tab_dev : (block + 1) * tab_dev]
            rows = pl.ds(block // 2 * tab_dev * pairs + pair, tab_dev, stride=pairs)

            @pl.when(side == block % 2)
            def _():
                kept_ref[rows, :] = value

            @pl.when(side != block % 2)
            def _():
                sent_ref[rows, :] = value


def make_bags(side, indices, lengths, line):
    micro, slots, batch, table_count = indices.shape
    shape = jax.ShapeDtypeStruct((table_count // 2 * (slots // 2), micro * batch), jnp.int32)
    return pl.pallas_call(
        functools.partial(bag_kernel, line),
        out_shape=(shape, shape),
        in_specs=[SMEM, VMEM, VMEM],
        out_specs=(VMEM, VMEM),
        compiler_params=params(32),
        cost_estimate=cost(6),
        name="bags",
    )(side[None], indices, lengths)


def turn_kernel(cuts, member_ref, tables_ref, *refs):
    outs, (held, sem) = refs[: len(cuts)], refs[len(cuts) :]
    size = held.shape[0]
    copy = pltpu.make_async_copy(tables_ref.at[pl.ds(member_ref[0] * size, size)], held, sem)
    copy.start()
    copy.wait()
    for table in range(size):
        turned = jnp.transpose(held[table])
        for (first, part), out in zip(cuts, outs):
            out[table] = turned[first : first + part]


def turn_piece(member, tables, size, cuts):
    _, rows, width = tables.shape
    return pl.pallas_call(
        functools.partial(turn_kernel, cuts),
        out_shape=[jax.ShapeDtypeStruct((size, part, rows), tables.dtype) for _, part in cuts],
        in_specs=[SMEM, ANY],
        out_specs=[VMEM] * len(cuts),
        scratch_shapes=[pltpu.VMEM((size, rows, width), tables.dtype), pltpu.SemaphoreType.DMA(())],
        compiler_params=params(63),
        cost_estimate=cost(3),
        name="turn",
    )(member[None], tables)


def bag_counts(bag, rows):
    bag = jnp.concatenate(
        [lax.shift_right_arithmetic(lax.shift_left(bag, 16), 16), lax.shift_right_arithmetic(bag, 16)],
        axis=0,
    )
    slots, samples = bag.shape
    span = rows // FIELDS
    word = bag & (span - 1)
    shift = lax.shift_right_logical(bag, span.bit_length() - 1) * BITS
    step = jnp.where(bag >= 0, lax.shift_left(jnp.ones_like(bag), shift & 31), 0)
    ids = lax.broadcasted_iota(jnp.int32, (span, samples), 0)
    packed = jnp.zeros((span, samples), jnp.int32)
    for slot in range(slots):
        packed = packed + jnp.where(ids == word[slot : slot + 1], step[slot : slot + 1], 0)
    fields = [
        (lax.shift_right_logical(packed, BITS * field) & (2**BITS - 1)).astype(jnp.float32)
        for field in range(FIELDS)
    ]
    return jnp.concatenate([field.astype(jnp.bfloat16) for field in fields], axis=0)


def pool_kernel(first, distances, pieces, size, unroll, earlier, own, places, *refs):
    sources = refs[: len(pieces)]
    bags_refs = refs[len(pieces) : len(pieces) + 2]
    refs = refs[len(pieces) + 2 :]
    before = refs[:earlier]
    refs = refs[earlier:]
    if earlier:
        project_ref, mine_ref, theirs_ref = refs[:3]
        tables_ref, bags, low_ref, high_ref, sems, sum_ref = refs[3:9]
        held = refs[9:]
        part = held[0].shape[0]
    else:
        (pooled_ref,) = refs[:1]
        tables_ref, bags, low_ref, high_ref, sems = refs[1:]
        part = pooled_ref.shape[0]
    count, blocks = tables_ref.shape[0], len(distances)
    tab_dev = count // blocks
    rows = tables_ref.shape[1 if own else 2]
    samples = bags.shape[3]
    stride = count + PAD
    halves = (low_ref, high_ref)
    member = places[1] * (0 if own else 1)

    soon, later = [], []
    for number, source in enumerate(bags_refs):
        for block in range(blocks):
            rows_from = source.at[pl.ds((places[0] ^ distances[block]) * tab_dev, tab_dev)]
            target = bags.at[number, pl.ds(block * tab_dev, tab_dev)]
            copy = pltpu.make_async_copy(rows_from, target, sems.at[number * blocks + block])
            (later if block else soon).append(copy)
    sem = 2 * blocks
    for source, (block, mask) in zip(sources, pieces):
        target = tables_ref.at[pl.ds(block * tab_dev + (member ^ mask) * size, size)]
        copy = pltpu.make_async_copy(source, target, sems.at[sem])
        (later if block or mask else soon).append(copy)
        sem += 1
    late = []
    for number, source in enumerate(before):
        columns = source.at[pl.ds(first if source.shape[0] != part else 0, part)]
        late.append(pltpu.make_async_copy(columns, held[number], sems.at[sem + number]))
    for copy in soon + later + late:
        copy.start()
    for copy in soon:
        copy.wait()

    base = member * size

    def some_tables(step, carry):
        if later:

            @pl.when(step == size // unroll)
            def _():
                for copy in later:
                    copy.wait()

        at = lax.rem(base + step * unroll, count)
        for inner in range(unroll):
            table = at + inner
            counts = jnp.concatenate(
                [bag_counts(bags[half, table], rows) for half in range(2)], axis=1
            )
            pooled = lax.dot_general(
                tables_ref[table],
                counts,
                (((0 if own else 1,), (0,)), ((), ())),
                preferred_element_type=jnp.float32,
            )
            for half in range(2):
                halves[half][pl.ds(table, part, stride=stride), :] = pooled[
                    :, half * samples : (half + 1) * samples
                ]
        return carry

    lax.fori_loop(0, count // unroll, some_tables, 0)

    if not earlier:

        def narrow(step, carry):
            for inner in range(16):
                column = step * 16 + inner
                start = pl.multiple_of(column * stride, PAD)
                for half in range(2):
                    value = halves[half][pl.ds(start, count), :].astype(jnp.bfloat16)
                    pooled_ref[column, :, half * samples : (half + 1) * samples] = value
            return carry

        lax.fori_loop(0, part // 16, narrow, 0)
        return

    outs = project_ref.shape[0]
    for copy in late:
        copy.wait()

    def some_columns(step, carry):
        for inner in range(16):
            column = step * 16 + inner
            start = pl.multiple_of(column * stride, PAD)
            here = [ref[pl.ds(start, count), :].astype(jnp.bfloat16) for ref in halves]
            pooled = jnp.concatenate(
                [ref[column] for ref in held] + [jnp.concatenate(here, axis=1)], axis=0
            )
            total = jnp.dot(project_ref[...], pooled, preferred_element_type=jnp.float32)
            mine_ref[pl.ds(column, outs, stride=part), :] = total[:, :samples]
            sum_ref[pl.ds(column, outs, stride=part), :] = total[:, samples:]
        return carry

    lax.fori_loop(0, part // 16, some_columns, 0)
    theirs_ref[...] = sum_ref[...].astype(theirs_ref.dtype)


def pool_blocks(
    places, distances, sources, pieces, bags, tab_dev, part, first=0, earlier=(), project=None
):
    own = distances == [0]
    blocks = len(distances)
    count = blocks * tab_dev
    size = sources[0].shape[0]
    rows = sources[0].shape[1 if own else 2]
    _, pairs, samples = bags[0].shape
    scratch = [
        pltpu.VMEM((count, rows, part) if own else (count, part, rows), jnp.bfloat16),
        pltpu.VMEM((2, count, pairs, samples), jnp.int32),
        pltpu.VMEM((part * (count + PAD), samples), jnp.float32),
        pltpu.VMEM((part * (count + PAD), samples), jnp.float32),
        pltpu.SemaphoreType.DMA((2 * blocks + len(pieces) + len(earlier),)),
    ]
    if earlier:
        outs = project.shape[0]
        out_shape = (
            jax.ShapeDtypeStruct((outs * part, samples), jnp.float32),
            jax.ShapeDtypeStruct((outs * part, samples), jnp.bfloat16),
        )
        out_specs = (VMEM, VMEM)
        scratch += [pltpu.VMEM((outs * part, samples), jnp.float32)]
        scratch += [pltpu.VMEM((part, *one.shape[1:]), jnp.bfloat16) for one in earlier]
        more, specs = (project,), [VMEM]
    else:
        out_shape = jax.ShapeDtypeStruct((part, count, 2 * samples), jnp.bfloat16)
        out_specs, more, specs = VMEM, (), []
    unroll = min(16, size)
    return pl.pallas_call(
        functools.partial(pool_kernel, first, distances, pieces, size, unroll, len(earlier), own),
        out_shape=out_shape,
        in_specs=[SMEM] + [ANY] * (len(sources) + 2 + len(earlier)) + specs,
        out_specs=out_specs,
        scratch_shapes=scratch,
        compiler_params=params(63),
        cost_estimate=cost(10),
        name="project" if earlier else "pool",
    )(places, *sources, *bags, *earlier, *more)


def score_kernel(masks, scale, member_ref, lead_ref, dense_ref, *refs):
    parts = len(refs) - len(masks) - 5
    sums = refs[:parts]
    top_parts = refs[parts : parts + len(masks)]
    scores_ref, turned, inter, top, sems = refs[parts + len(masks) :]
    own, back = sums[: parts // 2], sums[parts // 2 :]
    _, samples = dense_ref.shape
    outs = lead_ref.shape[0]
    half = outs // 2
    step_k, step_b = outs + PAD, samples + PAD
    copies = []
    for number, (mask, source) in enumerate(zip(masks, top_parts)):
        rows = source.shape[0]
        target = top.at[pl.ds((member_ref[0] ^ mask) * rows, rows)]
        copies.append(pltpu.make_async_copy(source, target, sems.at[number]))
    for copy in copies:
        copy.start()

    def compress(step, carry):
        for inner in range(8):
            k = step * 8 + inner
            columns = []
            for mine, theirs in zip(own, back):
                part = mine.shape[0] // outs
                rows = pl.ds(pl.multiple_of(k * part, part), part)
                columns.append(mine[rows, :] + theirs[rows, :].astype(jnp.float32))
            value = jnp.concatenate(columns, axis=0) + lead_ref[k] * dense_ref[...]
            value = jnp.transpose(value).astype(jnp.bfloat16).astype(jnp.float32)
            turned[pl.ds(k, samples, stride=step_k), :] = value
        return carry

    lax.fori_loop(0, outs // 8, compress, 0)

    def interact(step, carry):
        for inner in range(16):
            b = step * 16 + inner
            value = turned[pl.ds(pl.multiple_of(b * step_k, PAD), outs), :].astype(jnp.bfloat16)
            zero = jnp.zeros_like(value)
            left = jnp.concatenate([value[:half], value[half:]], axis=1)
            right = jnp.concatenate(
                [jnp.concatenate([value, zero], axis=1), jnp.concatenate([zero, value], axis=1)],
                axis=0,
            )
            pairs = lax.dot_general(
                left, right, (((1,), (1,)), ((), ())), preferred_element_type=jnp.float32
            )
            inter[pl.ds(b, half, stride=step_b), :] = pairs * scale
        return carry

    lax.fori_loop(0, samples // 16, interact, 0)
    for copy in copies:
        copy.wait()
    scores_ref[...] = jnp.zeros_like(scores_ref)

    def score(step, carry):
        left, right = [], []
        for inner in range(2):
            k = step * 2 + inner
            rows = pl.ds(pl.multiple_of(k * step_b, PAD), samples)
            left.append(inter[rows, :].astype(jnp.bfloat16))
            for high in range(2):
                start = pl.multiple_of((high * half + k) * outs, outs)
                right.append(top[pl.ds(start, outs), :])
        scores_ref[...] += jnp.dot(
            jnp.concatenate(left, axis=1),
            jnp.concatenate(right, axis=0),
            preferred_element_type=jnp.float32,
        )
        return carry

    lax.fori_loop(0, half // 2, score, 0)


def make_scores(place, lead, dense, own, back, tops, masks, top_shape):
    width, samples = dense.shape
    outs = lead.shape[0]
    return pl.pallas_call(
        functools.partial(score_kernel, masks, width ** (-0.5)),
        out_shape=jax.ShapeDtypeStruct((samples, top_shape[1]), jnp.float32),
        in_specs=[SMEM, SMEM, VMEM] + [VMEM] * (2 * len(own)) + [ANY] * len(tops),
        out_specs=VMEM,
        scratch_shapes=[
            pltpu.VMEM((samples * (outs + PAD), width), jnp.float32),
            pltpu.VMEM((outs // 2 * (samples + PAD), 2 * outs), jnp.float32),
            pltpu.VMEM(top_shape, jnp.bfloat16),
            pltpu.SemaphoreType.DMA((len(tops),)),
        ],
        compiler_params=params(40),
        cost_estimate=cost(20),
        name="scores",
    )(place, lead, dense, *own, *back, *tops)


def swap(value, axis, size, distance, keep=None, scale=1):
    pairs = []
    for a in range(size):
        if keep is None or keep(a, a ^ distance):
            pairs += [(a * scale + low, (a ^ distance) * scale + low) for low in range(scale)]
    return lax.ppermute(value, axis, pairs)


def routed_slot(distance):
    return distance >= 3 and distance % 2 == 1


def line_slot(value, slots, distance, line, position):
    if not routed_slot(distance):
        return swap(value, "emb", line, distance, None, 2)
    near = lambda a, b: abs(a - b) == 1
    direct = swap(value, "emb", line, distance, near, 2)
    far = lambda a, b: abs(b - (b ^ distance)) != 1
    routed = swap(slots[distance - 2], "emb", line, 1, far, 2)
    adjacent = jnp.abs(position - (position ^ distance)) == 1
    return jnp.where(adjacent, direct, routed)


def share(value, size):
    pieces, masks = [value], [0]
    for bit in bits_of(size):
        moved = [swap(piece, "grp", size, bit) for piece in pieces]
        pieces, masks = pieces + moved, masks + [mask ^ bit for mask in masks]
    return pieces, masks


def bits_of(size):
    return [2**power for power in range(size.bit_length() - 2, -1, -1)]


def chunk_widths(width, piece):
    return (width // 8 * SPLIT, width - width // 8 * SPLIT) if piece >= 4096 else (width,)


def shards(grp, emb, indices, lengths, dense, tables, project, top_weight):
    micro, slot_count, batch, _ = indices.shape
    tab_dev, rows, width = tables.shape
    outs = project.shape[0]
    samples = micro * batch
    line = emb // 2
    place = lax.axis_index("emb").astype(jnp.int32)
    member = lax.axis_index("grp").astype(jnp.int32)
    position, side = place // 2, place % 2
    size = tab_dev // grp
    cuts, first = [], 0
    for part in chunk_widths(width, size * rows):
        cuts.append((first, part))
        first += part
    sends = turn_piece(member, tables, size, cuts)

    top_rows = top_weight.shape[0]
    tops, top_masks = [top_weight], [0]
    for bit in bits_of(grp):
        moved = [swap(piece, "grp", grp, bit) for piece in tops]
        tops, top_masks = tops + moved, top_masks + [mask ^ bit for mask in top_masks]

    kept, sent = make_bags(side, indices, lengths, line)
    got = swap(sent, "emb", emb, 1)
    bags = [bag.reshape(line * tab_dev, slot_count // 2, samples) for bag in (kept, got)]

    mixing = project[:, 1:].reshape(outs, line, 2, tab_dev)
    mixing = lax.dynamic_index_in_dim(mixing, side, 2, keepdims=False)
    order = position ^ jnp.arange(line)
    mixing = jnp.take(mixing, order, axis=1).reshape(outs, line * tab_dev)

    mixing, where = lax.optimization_barrier((mixing, jnp.stack([position, member])))
    near = pool_blocks(where, [0], [tables], [(0, 0)], bags, tab_dev, width)
    own, back = [], []
    for chunk, ((first, part), send) in enumerate(zip(cuts, sends)):
        slots, sources, pieces = [], [], []
        for distance in range(1, line):
            slots.append(line_slot(send, slots, distance, line, position))
            shared, masks = share(slots[-1], grp)
            sources.append(shared)
            pieces.append([(0 if distance == line - 1 else distance - 1, mask) for mask in masks])
        pooled, groups = [near], [[distance] for distance in range(1, line - 1)]
        if chunk == len(cuts) - 1:
            groups = [sum(groups, [])] if groups else []
        for group in groups:
            arrays = sum([sources[distance - 1] for distance in group], [])
            marks = [(group.index(d), mask) for d in group for _, mask in pieces[d - 1]]
            pooled.append(pool_blocks(where, group, arrays, marks, bags, tab_dev, part))
        mine_sum, their_sum = pool_blocks(
            where,
            [line - 1],
            sources[-1],
            pieces[-1],
            bags,
            tab_dev,
            part,
            first,
            tuple(pooled),
            mixing,
        )
        own.append(mine_sum)
        back.append(swap(their_sum, "emb", emb, 1))

    flat_dense = jnp.transpose(dense.reshape(samples, width)).astype(jnp.float32)
    lead = project[:, 0].astype(jnp.float32)
    top_shape = (top_rows * grp, top_weight.shape[1])
    scores = make_scores(
        member[None], lead, flat_dense, own, back, tops, tuple(top_masks), top_shape
    )
    return scores.reshape(micro, batch, -1)


def solution(mesh):
    placed = (
        P(None, None, ("grp", "emb"), None),
        P(None, ("grp", "emb"), None),
        P(None, ("grp", "emb"), None),
        P("emb", None, None),
        P(),
        P("grp", None),
    )
    grp, emb = mesh.shape["grp"], mesh.shape["emb"]

    def body(*args):
        return shards(grp, emb, *args)

    step = jax.shard_map(
        body, mesh=mesh, in_specs=placed, out_specs=P(None, ("grp", "emb"), None), check_vma=False
    )

    def run(indices, lengths, dense, tables, project, top_weight):
        args = (indices, lengths, dense, tables, project, top_weight)
        return step(*args)

    return run
```
